32 devices in a mesh: grp: 4 (over y, core), vocab: 8 (over z, x).
Axes of the slice: x: 2, y: 2, z: 4, core: 2. Of those that a mesh axis runs over, the one named last changes fastest.
Arguments:
- hidden: bfloat16 [2048, 3584], P(('grp', 'vocab')), may hold values from -6 to 6
- embedding: bfloat16 [32768, 3584], P(('vocab', 'grp')), may hold values from -0.75 to 0.75
- targets: int32 [2048], P(('grp', 'vocab')), may hold values from 0 to 32767
- segments: int32 [2048], P(('grp', 'vocab')), may hold values from 0 to 15, never falling along the last dimension, each value on 1 to 256 neighbouring positions
Outputs:
- token_loss: float32 [2048], P(('grp', 'vocab'))
- doc_zloss: float32 [16], replicated
The draws below stay inside these ranges and needn't reach their ends.
Inputs may be any that keep to these rules, and one draw needn't show every extreme that they name: `segments`: segment ids never fall along the tokens; each document has 1 to 256 tokens.
All inputs are finite; a program needn't handle non-finite values.
Results may differ from the reference program's by a relative error of at most 0.0003.
Values may be sent and summed in bfloat16 or wider, within the bound.
A program may use at most 128 MiB of HBM per device.

```python
import math
import jax
import jax.numpy as jnp
import numpy as np
from jax import lax

D = 3584
VOCAB_DEV = 4096
TOK_GRP = 512
DOC_GRP = 4
VOCAB = 32768
TOKENS = 2048
DOCS = 16
N_VOCAB = 8


def place_ends(result, stream_key, low, top_value):
    shape = result.shape
    index_at = [jax.random.randint(jax.random.fold_in(stream_key, axis), (), 0, shape[axis]) for axis in range(len(shape))]
    result = result.at[tuple(index_at)].set(low)
    longest = shape.index(max(shape))
    index_at[longest] = (index_at[longest] + 1) % shape[longest]
    return result.at[tuple(index_at)].set(top_value)


def steps_of(stream_key, shape, pieces, smallest, largest):
    factor_of, own = 1.0, jax.random.fold_in(stream_key, 6)
    for dim, parts in pieces:
        steps = jnp.exp(jax.random.uniform(jax.random.fold_in(own, dim), (parts,), jnp.float32, smallest / len(pieces), largest / len(pieces)))
        factor_of = factor_of * jnp.repeat(steps, shape[dim] // parts).reshape([-1 if axis == dim else 1 for axis in range(len(shape))])
    return factor_of


def split_up(number_of, total, most, slope):
    portions = [(1 << 20) // math.isqrt(rank ** slope) + 1 for rank in range(2, number_of + 1)]
    rest, given = total - most - (number_of - 1), [1] * (number_of - 1)
    while rest > 0:
        candidates = [i for i in range(number_of - 1) if given[i] < most]
        mass, left = sum([portions[i] for i in candidates]), rest
        for i in candidates:
            addition = min(most - given[i], max(1, left * portions[i] // mass), rest)
            given[i] = given[i] + addition
            rest = rest - addition
    return np.array([most] + given)


def ragged(key, amount, total, reach, slope):
    if amount == 2:
        one = jax.random.randint(key, (), max(1, total - reach), min(reach, total - 1) + 1)
        return jnp.stack([one, total - one])
    sizes = jnp.asarray(split_up(amount, total, reach, slope), jnp.int32)
    twos = (amount - 1) // 2
    giver, sink = sizes[1:1 + 2 * twos:2], sizes[2:2 + 2 * twos:2]
    margin = jnp.minimum(giver - 1, reach - sink)
    shifted = jax.random.randint(jax.random.fold_in(key, 1), (twos,), 0, 1 << 20) % (margin + 1)
    sizes = sizes.at[1:1 + 2 * twos:2].set(giver - shifted).at[2:2 + 2 * twos:2].set(sink + shifted)
    return sizes[jax.random.permutation(jax.random.fold_in(key, 2), amount)]


def scatter_about(own_key, extent, spread, most, pieces=(), kind=jnp.bfloat16):
    entries = spread * jax.random.normal(own_key, extent, jnp.float32)
    if pieces:
        entries = entries * steps_of(own_key, extent, pieces, -0.22, 0.18)
    return jnp.clip(entries, -most, most).astype(kind)


def setup_inputs(seed: int = 0) -> dict:
    splits = jax.random.split(jax.random.key(seed), 5)
    hidden = scatter_about(splits[0], (TOKENS, D), 1.0, 6.0, ((0, 32),))
    embedding = scatter_about(splits[1], (VOCAB, D), (D // 64) ** -0.5, 0.75, ((0, 32),))
    targets = place_ends(jax.random.randint(splits[2], (TOKENS,), 0, VOCAB), jax.random.fold_in(splits[2], 1), 0, VOCAB - 1).astype(jnp.int32)
    segments = jnp.searchsorted(jnp.cumsum(ragged(splits[3], DOCS, TOKENS, 2 * TOK_GRP // DOC_GRP, 1)), jnp.arange(TOKENS), side="right").astype(jnp.int32)
    return dict(hidden=hidden, embedding=embedding, targets=targets, segments=segments)


soft_cap = 30.0
zloss_coef = 0.0001


def reference(hidden, embedding, targets, segments):
    def block(carry, index):
        start = index * VOCAB_DEV
        rows = lax.dynamic_slice_in_dim(embedding, start, VOCAB_DEV, 0)
        logits = lax.dot_general(hidden, rows, (((1,), (1,)), ((), ())), preferred_element_type=jnp.float32)
        capped = soft_cap * jnp.tanh(logits / soft_cap)
        sumexp = jnp.sum(jnp.exp(capped - soft_cap), axis=1)
        idents = start + jnp.arange(VOCAB_DEV, dtype=jnp.int32)
        hit = idents[None, :] == targets[:, None]
        picked = jnp.sum(jnp.where(hit, capped, jnp.zeros_like(capped)), axis=1)
        return (carry[0] + sumexp, carry[1] + picked), None

    zeros = jnp.zeros((TOKENS,), jnp.float32)
    (total, picked), _ = lax.scan(block, (zeros, zeros), jnp.arange(N_VOCAB, dtype=jnp.int32))
    lse = soft_cap + jnp.log(total)
    zterm = zloss_coef * lse * lse
    token_loss = lse - picked + zterm
    onehot = (segments[:, None] == jnp.arange(DOCS, dtype=jnp.int32)[None, :]).astype(jnp.float32)
    doc_zloss = jnp.dot(zterm, onehot, precision=lax.Precision.HIGHEST)
    return token_loss, doc_zloss
```

```python
import functools

import jax
import jax.numpy as jnp
from jax import lax
from jax.experimental import pallas as pl
from jax.experimental.pallas import tpu as pltpu
from jax.sharding import PartitionSpec as P

DOC_GRP = 4
LANES = 128
CORES = 2
MESH = pl.DeviceIdType.MESH

soft_cap = 30.0
zloss_coef = 0.0001


def kernel(dims, hid_ref, emb_ref, tgt_ref, seg_ref, loss_ref, doc_ref, buf, emb, tgs, sums, parts, docs,
           local_sem, send_sem, recv_sem, small_send, small_recv):
    NA, NB, Z, X, V, N, U, chunk = dims
    nb, rows, depth = buf.shape
    R = rows // U
    shard = emb.shape[0]
    n_docs = doc_ref.shape[1]
    g, v = lax.axis_index("grp"), lax.axis_index("vocab")
    me = g * V + v
    core, y, x, z = g % CORES, g // CORES, v % X, v // X
    swap = NA == NB

    def turn(c, p, q):
        return (jnp.where(c == 0, p, q), jnp.where(c == 0, q, p)) if swap else (p, q)

    a, b = turn(core, x, y)

    def device(c, aa, bb, zz):
        xx, yy = turn(c, aa, bb)
        return (yy * CORES + c, zz * X + xx)

    def pos(c, aa, bb, zz):
        return ((c * Z + zz) * NB + bb) * NA + aa

    def natural(c, aa, bb, zz):
        gg, vv = device(c, aa, bb, zz)
        return gg * V + vv

    def other(k):
        t = (me + k) % N
        return (t // V, t % V), t

    own = pos(core, a, b, z)
    load_hid = pltpu.make_async_copy(hid_ref, buf.at[own], local_sem.at[0])
    load_emb = pltpu.make_async_copy(emb_ref, emb, local_sem.at[1])
    load_tgt = pltpu.make_async_copy(tgt_ref, tgs.at[me], local_sem.at[2])
    load_hid.start()
    load_tgt.start()

    barrier = pltpu.get_barrier_semaphore()

    @pl.loop(1, N)
    def _(k):
        pl.semaphore_signal(barrier, inc=1, device_id=other(k)[0], device_id_type=MESH)

    load_emb.start()
    load_hid.wait()
    load_tgt.wait()
    pl.semaphore_wait(barrier, N - 1)

    def copy(p, u, d, dev):
        piece = buf.at[p, pl.ds(u * R, R)]
        return pltpu.make_async_remote_copy(
            piece, piece, send_sem.at[p * U + u, d], recv_sem.at[p * U + u], device_id=dev, device_id_type=MESH
        )

    def traverse(start):
        def put(p, u, d, at, size, dev):
            @pl.when((at >= 0) & (at < size))
            def _():
                c = copy(p, u, d, dev(at))
                c.start() if start else c.wait_send()

        def z_way(p, u, d, sgn):
            put(p, u, d, z + sgn, Z, lambda w: device(core, a, b, w))

        def a_way(p, u, d, sgn):
            put(p, u, d, a + sgn, NA, lambda w: device(core, w, b, z))

        def b_way(p, u, d, sgn):
            put(p, u, d, b + sgn, NB, lambda w: device(core, a, w, z))

        def twin(p, u):
            c = copy(p, u, 6, device_of_twin)
            c.start() if start else c.wait_send()

        def z_both(p, u):
            z_way(p, u, 0, 1)
            z_way(p, u, 1, -1)

        def a_both(p, u):
            a_way(p, u, 2, 1)
            a_way(p, u, 3, -1)

        def b_both(p, u):
            b_way(p, u, 4, 1)
            b_way(p, u, 5, -1)

        def arrive(p, u):
            if start:
                copy(p, u, 6, device_of_twin).wait_recv()

        if U > 1:
            a_both(own, 1)
        z_both(own, 0)
        b_both(own, 0)
        a_both(own, 0)
        if U > 1:
            z_both(own, 1)
            b_both(own, 1)
        for u in range(U):
            twin(own, u)

        def across_a(zz, u, extra):
            for da in range(1, NA):
                for sgn in (1, -1):
                    at = a + sgn * da

                    @pl.when((at >= 0) & (at < NA))
                    def _():
                        p = pos(core, at, b, zz)
                        arrive(p, u)
                        a_way(p, u, 2 if sgn < 0 else 3, -sgn)
                        if extra:
                            z_both(p, u)
                        b_both(p, u)
                        twin(p, u)

        def sides(s, fn):
            @pl.loop(0, 2)
            def _(side):
                zz = z + (1 - 2 * side) * s

                @pl.when((zz >= 0) & (zz < Z) & ((s > 0) | (side == 0)))
                def _():
                    fn(zz, side)

        if U > 1:
            across_a(z, 1, True)

        def z_arrivals(zz, side):
            onward = 2 * side - 1

            def one(p, u):
                arrive(p, u)
                put(p, u, 1 - side, z + onward, Z, lambda w: device(core, a, b, w))

            p = pos(core, a, b, zz)
            one(p, 0)
            a_both(p, 0)
            b_both(p, 0)
            twin(p, 0)
            for u in range(1, U):
                @pl.loop(0, NA)
                def _(k):
                    q = pos(core, (a + k) % NA, b, zz)
                    one(q, u)
                    b_both(q, u)
                    twin(q, u)

        def late(zz, side):
            across_a(zz, 0, False)

        def b_arrivals(zz, side):
            for u in range(U):
                @pl.loop(0, NA)
                def _(k):
                    for db in range(1, NB):
                        for sgn in (1, -1):
                            at = b + sgn * db

                            @pl.when((at >= 0) & (at < NB))
                            def _():
                                p = pos(core, (a + k) % NA, at, zz)
                                arrive(p, u)
                                b_way(p, u, 4 if sgn < 0 else 5, -sgn)
                                twin(p, u)

        @pl.loop(1, Z + 1)
        def _(s):
            @pl.when(s < Z)
            def _():
                sides(s, z_arrivals)

            sides(s - 1, late)
            sides(s - 1, b_arrivals)
            if start:
                @pl.when(s == 1)
                def _():
                    load_emb.wait()
                    few = tgs.at[pl.ds(0, N - 1)]
                    pltpu.make_async_remote_copy(
                        few, few, small_send.at[0], small_recv.at[0], device_id=device_of_twin, device_id_type=MESH
                    ).wait()

                sides(s - 1, batch)

    device_of_twin = ((g // CORES) * CORES + 1 - core, v)

    @pl.loop(1, N)
    def _(k):
        pltpu.make_async_remote_copy(
            tgs.at[me], tgs.at[me], small_send.at[0], small_recv.at[0], device_id=other(k)[0], device_id_type=MESH
        ).start()

    blocks = NA * NB
    first_id = (v * lax.axis_size("grp") + g) * shard

    def batch(zz, side):
        @pl.loop(0, CORES)
        def _(k):
            c = (core + k) % CORES
            base = pos(c, 0, 0, zz)

            @pl.when(k == 1)
            def _():
                @pl.loop(0, blocks * U)
                def _(i):
                    copy(base + i // U, i % U, 6, device_of_twin).wait_recv()

            where_to = [natural(c, i % NA, i // NA, zz) for i in range(blocks)]
            wanted = jnp.concatenate([tgs[w] for w in where_to], axis=1)
            tokens = blocks * rows

            def step(i, carry):
                start = pl.multiple_of(i * chunk, chunk)
                logits = lax.dot_general(
                    emb[pl.ds(start, chunk), :],
                    buf[pl.ds(base, blocks)].reshape(tokens, depth),
                    (((1,), (1,)), ((), ())),
                    preferred_element_type=jnp.float32,
                )
                capped = soft_cap * jnp.tanh(logits * (1.0 / soft_cap))
                ids = lax.broadcasted_iota(jnp.int32, (chunk, tokens), 0)
                hit = ids == (wanted - (first_id + start))
                return (
                    carry[0] + jnp.sum(jnp.exp(capped - soft_cap), axis=0, keepdims=True),
                    carry[1] + jnp.sum(jnp.where(hit, capped, 0.0), axis=0, keepdims=True),
                )

            zero = jnp.zeros((1, tokens), jnp.float32)
            total, picked = lax.fori_loop(0, shard // chunk, step, (zero, zero))
            for i, w in enumerate(where_to):
                sums[w, 0:1, :] = total[:, i * rows : (i + 1) * rows]
                sums[w, 1:2, :] = picked[:, i * rows : (i + 1) * rows]

    traverse(True)

    def exchange(source_of, dest, which):
        @pl.loop(1, N)
        def _(k):
            dev, t = other(k)
            pltpu.make_async_remote_copy(
                source_of(t), dest.at[me], small_send.at[which], small_recv.at[which], device_id=dev, device_id_type=MESH
            ).start()

    def settle(dest, which):
        few = dest.at[pl.ds(0, N - 1)]
        pltpu.make_async_remote_copy(
            few, few, small_send.at[which], small_recv.at[which], device_id=device_of_twin, device_id_type=MESH
        ).wait()

    exchange(lambda t: sums.at[t], parts, 1)
    parts[me] = sums[me]
    traverse(False)
    settle(parts, 1)

    both = jnp.sum(parts[...], axis=0)
    lse = soft_cap + jnp.log(both[0:1, :])
    zterm = zloss_coef * lse * lse
    loss_ref[...] = lse - both[1:2, :] + zterm
    width = docs.shape[2]
    of_doc = lax.broadcasted_iota(jnp.int32, (n_docs, rows), 0) == seg_ref[...]
    column = jnp.sum(jnp.where(of_doc, zterm, 0.0), axis=1, keepdims=True)
    diagonal = lax.broadcasted_iota(jnp.int32, (n_docs, width), 0) == lax.broadcasted_iota(
        jnp.int32, (n_docs, width), 1
    )
    docs[me] = jnp.sum(jnp.where(diagonal, column, 0.0), axis=0, keepdims=True)
    exchange(lambda t: docs.at[me], docs, 2)
    settle(docs, 2)
    doc_ref[...] = jnp.sum(docs[...], axis=0)[:, :n_docs]


def solution(mesh):
    G, V = mesh.shape["grp"], mesh.shape["vocab"]
    N = G * V
    Y = G // CORES
    X = Y if V % Y == 0 else 1
    Z = V // X
    n_docs = DOC_GRP * G

    def body(hidden, embedding, targets, segments):
        rows, depth = hidden.shape
        shard = embedding.shape[0]
        U = 2 if rows % 32 == 0 else 1
        chunk = min(512, shard)
        dims = (X, Y, Z, X, V, N, U, chunk)
        width = -(-n_docs // LANES) * LANES
        any_spec = pl.BlockSpec(memory_space=pl.ANY)
        vmem = pl.BlockSpec(memory_space=pltpu.VMEM)
        loss, doc = pl.pallas_call(
            functools.partial(kernel, dims),
            out_shape=(
                jax.ShapeDtypeStruct((1, rows), jnp.float32),
                jax.ShapeDtypeStruct((1, n_docs), jnp.float32),
            ),
            in_specs=[any_spec, any_spec, vmem, vmem],
            out_specs=(vmem, vmem),
            scratch_shapes=[
                pltpu.VMEM((N, rows, depth), jnp.bfloat16),
                pltpu.VMEM((shard, depth), jnp.bfloat16),
                pltpu.VMEM((N, 1, rows), jnp.int32),
                pltpu.VMEM((N, 2, rows), jnp.float32),
                pltpu.VMEM((N, 2, rows), jnp.float32),
                pltpu.VMEM((N, 1, width), jnp.float32),
                pltpu.SemaphoreType.DMA((3,)),
                pltpu.SemaphoreType.DMA((N * U, 7)),
                pltpu.SemaphoreType.DMA((N * U,)),
                pltpu.SemaphoreType.DMA((3,)),
                pltpu.SemaphoreType.DMA((3,)),
            ],
            compiler_params=pltpu.CompilerParams(
                collective_id=0, has_side_effects=True, vmem_limit_bytes=60 * 1024 * 1024
            ),
        )(hidden, embedding, targets.reshape(1, rows), segments.reshape(1, rows))
        return (loss.reshape(rows), doc.reshape(n_docs))

    return jax.shard_map(
        body,
        mesh=mesh,
        in_specs=(
            P(("grp", "vocab"), None),
            P(("vocab", "grp"), None),
            P(("grp", "vocab")),
            P(("grp", "vocab")),
        ),
        out_specs=(P(("grp", "vocab")), P()),
        check_vma=False,
    )
```

```python
import functools

import jax
import jax.numpy as jnp
from jax import lax
from jax.experimental import pallas as pl
from jax.experimental.pallas import tpu as pltpu
from jax.sharding import PartitionSpec as P

DOC_GRP = 4
LANES = 128
CORES = 2
MESH = pl.DeviceIdType.MESH

soft_cap = 30.0
zloss_coef = 0.0001


def kernel(dims, hid_ref, emb_ref, tgt_ref, seg_ref, loss_ref, doc_ref, buf, emb, tgs, sums, parts, docs,
           local_sem, send_sem, recv_sem, small_send, small_recv):
    NA, NB, Z, X, V, N, U, chunk = dims
    nb, rows, depth = buf.shape
    R = rows // U
    shard = emb.shape[0]
    n_docs = doc_ref.shape[1]
    g, v = lax.axis_index("grp"), lax.axis_index("vocab")
    me = g * V + v
    core, y, x, z = g % CORES, g // CORES, v % X, v // X
    swap = NA == NB

    def turn(c, p, q):
        return (jnp.where(c == 0, p, q), jnp.where(c == 0, q, p)) if swap else (p, q)

    a, b = turn(core, x, y)

    def device(c, aa, bb, zz):
        xx, yy = turn(c, aa, bb)
        return (yy * CORES + c, zz * X + xx)

    def pos(c, aa, bb, zz):
        return ((c * Z + zz) * NB + bb) * NA + aa

    def natural(c, aa, bb, zz):
        gg, vv = device(c, aa, bb, zz)
        return gg * V + vv

    def other(k):
        t = (me + k) % N
        return (t // V, t % V), t

    own = pos(core, a, b, z)
    load_hid = pltpu.make_async_copy(hid_ref, buf.at[own], local_sem.at[0])
    load_emb = pltpu.make_async_copy(emb_ref, emb, local_sem.at[1])
    load_tgt = pltpu.make_async_copy(tgt_ref, tgs.at[me], local_sem.at[2])
    load_hid.start()
    load_tgt.start()

    barrier = pltpu.get_barrier_semaphore()

    @pl.loop(1, N)
    def _(k):
        pl.semaphore_signal(barrier, inc=1, device_id=other(k)[0], device_id_type=MESH)

    load_emb.start()
    load_hid.wait()
    load_tgt.wait()
    pl.semaphore_wait(barrier, N - 1)

    def copy(p, u, d, dev):
        piece = buf.at[p, pl.ds(u * R, R)]
        return pltpu.make_async_remote_copy(
            piece, piece, send_sem.at[p * U + u, d], recv_sem.at[p * U + u], device_id=dev, device_id_type=MESH
        )

    def traverse(start):
        def put(p, u, d, at, size, dev):
            @pl.when((at >= 0) & (at < size))
            def _():
                c = copy(p, u, d, dev(at))
                c.start() if start else c.wait_send()

        def z_way(p, u, d, sgn):
            put(p, u, d, z + sgn, Z, lambda w: device(core, a, b, w))

        def a_way(p, u, d, sgn):
            put(p, u, d, a + sgn, NA, lambda w: device(core, w, b, z))

        def b_way(p, u, d, sgn):
            put(p, u, d, b + sgn, NB, lambda w: device(core, a, w, z))

        def twin(p, u):
            c = copy(p, u, 6, device_of_twin)
            c.start() if start else c.wait_send()

        def z_both(p, u):
            z_way(p, u, 0, 1)
            z_way(p, u, 1, -1)

        def mid_way(p, u, sgn):
            (a_way if u == 0 else b_way)(p, u, 2 if sgn > 0 else 3, sgn)

        def last_way(p, u, sgn):
            (b_way if u == 0 else a_way)(p, u, 4 if sgn > 0 else 5, sgn)

        def mid_both(p, u):
            mid_way(p, u, 1)
            mid_way(p, u, -1)

        def last_both(p, u):
            last_way(p, u, 1)
            last_way(p, u, -1)

        def role(u):
            return (a, NA, b, NB) if u == 0 else (b, NB, a, NA)

        def at_role(u, mid, last, zz):
            return pos(core, mid, last, zz) if u == 0 else pos(core, last, mid, zz)

        def arrive(p, u):
            if start:
                copy(p, u, 6, device_of_twin).wait_recv()

        if U > 1:
            mid_both(own, 1)
        z_both(own, 0)
        last_both(own, 0)
        mid_both(own, 0)
        if U > 1:
            z_both(own, 1)
            last_both(own, 1)
        for u in range(U):
            twin(own, u)

        def across_mid(zz, u, extra):
            here, size, last, _ = role(u)
            for step in range(1, size):
                for sgn in (1, -1):
                    at = here + sgn * step

                    @pl.when((at >= 0) & (at < size))
                    def _():
                        p = at_role(u, at, last, zz)
                        arrive(p, u)
                        mid_way(p, u, -sgn)
                        if extra:
                            z_both(p, u)
                        last_both(p, u)
                        twin(p, u)

        def sides(s, fn):
            @pl.loop(0, 2)
            def _(side):
                zz = z + (1 - 2 * side) * s

                @pl.when((zz >= 0) & (zz < Z) & ((s > 0) | (side == 0)))
                def _():
                    fn(zz, side)

        if U > 1:
            across_mid(z, 1, True)

        def from_z(p, u, side):
            arrive(p, u)
            put(p, u, 1 - side, z + 2 * side - 1, Z, lambda w: device(core, a, b, w))

        def z_first(zz, side):
            p = pos(core, a, b, zz)
            from_z(p, 0, side)
            mid_both(p, 0)
            last_both(p, 0)
            twin(p, 0)

        def z_second(zz, side, k, u):
            here, size, last, _ = role(u)
            q = at_role(u, (here + k) % size, last, zz)
            from_z(q, u, side)
            last_both(q, u)
            twin(q, u)

        def late(zz, side):
            across_mid(zz, 0, False)

        def b_arrivals(zz, side):
            for u in range(U):
                here, size, last, length = role(u)

                @pl.loop(0, size)
                def _(k):
                    for step in range(1, length):
                        for sgn in (1, -1):
                            at = last + sgn * step

                            @pl.when((at >= 0) & (at < length))
                            def _():
                                p = at_role(u, (here + k) % size, at, zz)
                                arrive(p, u)
                                last_way(p, u, -sgn)
                                twin(p, u)

        @pl.loop(1, Z + 2)
        def _(s):
            @pl.when(s < Z)
            def _():
                sides(s, z_first)
                for u in range(1, U):
                    @pl.loop(0, role(u)[1])
                    def _(k):
                        sides(s, lambda zz, side: z_second(zz, side, k, u))

            @pl.when(s <= Z)
            def _():
                sides(s - 1, late)

            @pl.when(s >= 2)
            def _():
                sides(s - 2, b_arrivals)
                if start:
                    @pl.when(s == 2)
                    def _():
                        load_emb.wait()
                        few = tgs.at[pl.ds(0, N - 1)]
                        pltpu.make_async_remote_copy(
                            few, few, small_send.at[0], small_recv.at[0], device_id=device_of_twin, device_id_type=MESH
                        ).wait()

                    sides(s - 2, batch)

    device_of_twin = ((g // CORES) * CORES + 1 - core, v)

    @pl.loop(1, N)
    def _(k):
        pltpu.make_async_remote_copy(
            tgs.at[me], tgs.at[me], small_send.at[0], small_recv.at[0], device_id=other(k)[0], device_id_type=MESH
        ).start()

    blocks = NA * NB
    first_id = (v * lax.axis_size("grp") + g) * shard

    def batch(zz, side):
        @pl.loop(0, CORES)
        def _(k):
            c = (core + k) % CORES
            base = pos(c, 0, 0, zz)

            @pl.when(k == 1)
            def _():
                @pl.loop(0, blocks * U)
                def _(i):
                    copy(base + i // U, i % U, 6, device_of_twin).wait_recv()

            where_to = [natural(c, i % NA, i // NA, zz) for i in range(blocks)]
            wanted = jnp.concatenate([tgs[w] for w in where_to], axis=1)
            tokens = blocks * rows

            def step(i, carry):
                start = pl.multiple_of(i * chunk, chunk)
                logits = lax.dot_general(
                    emb[pl.ds(start, chunk), :],
                    buf[pl.ds(base, blocks)].reshape(tokens, depth),
                    (((1,), (1,)), ((), ())),
                    preferred_element_type=jnp.float32,
                )
                capped = soft_cap * jnp.tanh(logits * (1.0 / soft_cap))
                ids = lax.broadcasted_iota(jnp.int32, (chunk, tokens), 0)
                hit = ids == (wanted - (first_id + start))
                return (
                    carry[0] + jnp.sum(jnp.exp(capped - soft_cap), axis=0, keepdims=True),
                    carry[1] + jnp.sum(jnp.where(hit, capped, 0.0), axis=0, keepdims=True),
                )

            zero = jnp.zeros((1, tokens), jnp.float32)
            total, picked = lax.fori_loop(0, shard // chunk, step, (zero, zero))
            for i, w in enumerate(where_to):
                sums[w, 0:1, :] = total[:, i * rows : (i + 1) * rows]
                sums[w, 1:2, :] = picked[:, i * rows : (i + 1) * rows]
            for w in where_to:
                @pl.when(w != me)
                def _():
                    pltpu.make_async_remote_copy(
                        sums.at[w], parts.at[me], small_send.at[1], small_recv.at[1],
                        device_id=(w // V, w % V), device_id_type=MESH,
                    ).start()

    traverse(True)

    def exchange(source_of, dest, which):
        @pl.loop(1, N)
        def _(k):
            dev, t = other(k)
            pltpu.make_async_remote_copy(
                source_of(t), dest.at[me], small_send.at[which], small_recv.at[which], device_id=dev, device_id_type=MESH
            ).start()

    def settle(dest, which):
        few = dest.at[pl.ds(0, N - 1)]
        pltpu.make_async_remote_copy(
            few, few, small_send.at[which], small_recv.at[which], device_id=device_of_twin, device_id_type=MESH
        ).wait()

    parts[me] = sums[me]
    traverse(False)
    settle(parts, 1)

    both = jnp.sum(parts[...], axis=0)
    lse = soft_cap + jnp.log(both[0:1, :])
    zterm = zloss_coef * lse * lse
    loss_ref[...] = lse - both[1:2, :] + zterm
    width = docs.shape[2]
    of_doc = lax.broadcasted_iota(jnp.int32, (n_docs, rows), 0) == seg_ref[...]
    column = jnp.sum(jnp.where(of_doc, zterm, 0.0), axis=1, keepdims=True)
    diagonal = lax.broadcasted_iota(jnp.int32, (n_docs, width), 0) == lax.broadcasted_iota(
        jnp.int32, (n_docs, width), 1
    )
    docs[me] = jnp.sum(jnp.where(diagonal, column, 0.0), axis=0, keepdims=True)
    exchange(lambda t: docs.at[me], docs, 2)
    settle(docs, 2)
    doc_ref[...] = jnp.sum(docs[...], axis=0)[:, :n_docs]


def solution(mesh):
    G, V = mesh.shape["grp"], mesh.shape["vocab"]
    N = G * V
    Y = G // CORES
    X = Y if V % Y == 0 else 1
    Z = V // X
    n_docs = DOC_GRP * G

    def body(hidden, embedding, targets, segments):
        rows, depth = hidden.shape
        shard = embedding.shape[0]
        U = 2 if rows % 32 == 0 else 1
        chunk = min(1024, shard)
        dims = (X, Y, Z, X, V, N, U, chunk)
        width = -(-n_docs // LANES) * LANES
        any_spec = pl.BlockSpec(memory_space=pl.ANY)
        vmem = pl.BlockSpec(memory_space=pltpu.VMEM)
        loss, doc = pl.pallas_call(
            functools.partial(kernel, dims),
            out_shape=(
                jax.ShapeDtypeStruct((1, rows), jnp.float32),
                jax.ShapeDtypeStruct((1, n_docs), jnp.float32),
            ),
            in_specs=[any_spec, any_spec, vmem, vmem],
            out_specs=(vmem, vmem),
            scratch_shapes=[
                pltpu.VMEM((N, rows, depth), jnp.bfloat16),
                pltpu.VMEM((shard, depth), jnp.bfloat16),
                pltpu.VMEM((N, 1, rows), jnp.int32),
                pltpu.VMEM((N, 2, rows), jnp.float32),
                pltpu.VMEM((N, 2, rows), jnp.float32),
                pltpu.VMEM((N, 1, width), jnp.float32),
                pltpu.SemaphoreType.DMA((3,)),
                pltpu.SemaphoreType.DMA((N * U, 7)),
                pltpu.SemaphoreType.DMA((N * U,)),
                pltpu.SemaphoreType.DMA((3,)),
                pltpu.SemaphoreType.DMA((3,)),
            ],
            compiler_params=pltpu.CompilerParams(
                collective_id=0, has_side_effects=True, vmem_limit_bytes=60 * 1024 * 1024
            ),
        )(hidden, embedding, targets.reshape(1, rows), segments.reshape(1, rows))
        return (loss.reshape(rows), doc.reshape(n_docs))

    return jax.shard_map(
        body,
        mesh=mesh,
        in_specs=(
            P(("grp", "vocab"), None),
            P(("vocab", "grp"), None),
            P(("grp", "vocab")),
            P(("grp", "vocab")),
        ),
        out_specs=(P(("grp", "vocab")), P()),
        check_vma=False,
    )
```

```python
import functools

import jax
import jax.numpy as jnp
from jax import lax
from jax.experimental import pallas as pl
from jax.experimental.pallas import tpu as pltpu
from jax.sharding import PartitionSpec as P

DOC_GRP = 4
LANES = 128
CORES = 2
MESH = pl.DeviceIdType.MESH

soft_cap = 30.0
zloss_coef = 0.0001


def kernel(dims, hid_ref, emb_ref, tgt_ref, seg_ref, loss_ref, doc_ref, buf, emb, tgs, sums, parts, docs,
           local_sem, send_sem, recv_sem, small_send, small_recv):
    NA, NB, Z, X, V, N, U, chunk = dims
    nb, rows, depth = buf.shape
    R = rows // U
    shard = emb.shape[0]
    n_docs = doc_ref.shape[1]
    g, v = lax.axis_index("grp"), lax.axis_index("vocab")
    me = g * V + v
    core, y, x, z = g % CORES, g // CORES, v % X, v // X
    swap = NA == NB

    def turn(c, p, q):
        return (jnp.where(c == 0, p, q), jnp.where(c == 0, q, p)) if swap else (p, q)

    a, b = turn(core, x, y)

    def device(c, aa, bb, zz):
        xx, yy = turn(c, aa, bb)
        return (yy * CORES + c, zz * X + xx)

    def pos(c, aa, bb, zz):
        return ((c * Z + zz) * NB + bb) * NA + aa

    def natural(c, aa, bb, zz):
        gg, vv = device(c, aa, bb, zz)
        return gg * V + vv

    def other(k):
        t = (me + k) % N
        return (t // V, t % V), t

    own = pos(core, a, b, z)
    load_hid = pltpu.make_async_copy(hid_ref, buf.at[own], local_sem.at[0])
    load_emb = pltpu.make_async_copy(emb_ref, emb, local_sem.at[1])
    load_tgt = pltpu.make_async_copy(tgt_ref, tgs.at[me], local_sem.at[2])
    load_hid.start()
    load_tgt.start()

    barrier = pltpu.get_barrier_semaphore()

    @pl.loop(1, N)
    def _(k):
        pl.semaphore_signal(barrier, inc=1, device_id=other(k)[0], device_id_type=MESH)

    load_emb.start()
    load_hid.wait()
    load_tgt.wait()
    pl.semaphore_wait(barrier, N - 1)

    def copy(p, u, d, dev):
        piece = buf.at[p, pl.ds(u * R, R)]
        return pltpu.make_async_remote_copy(
            piece, piece, send_sem.at[p * U + u, d], recv_sem.at[p * U + u], device_id=dev, device_id_type=MESH
        )

    def send_targets():
        @pl.loop(1, N)
        def _(k):
            pltpu.make_async_remote_copy(
                tgs.at[me], tgs.at[me], small_send.at[0], small_recv.at[0], device_id=other(k)[0], device_id_type=MESH
            ).start()

    def traverse(start):
        def put(p, u, d, at, size, dev):
            @pl.when((at >= 0) & (at < size))
            def _():
                c = copy(p, u, d, dev(at))
                c.start() if start else c.wait_send()

        def z_way(p, u, d, sgn):
            put(p, u, d, z + sgn, Z, lambda w: device(core, a, b, w))

        def a_way(p, u, d, sgn):
            put(p, u, d, a + sgn, NA, lambda w: device(core, w, b, z))

        def b_way(p, u, d, sgn):
            put(p, u, d, b + sgn, NB, lambda w: device(core, a, w, z))

        def twin(p, u):
            c = copy(p, u, 6, device_of_twin)
            c.start() if start else c.wait_send()

        def z_both(p, u):
            z_way(p, u, 0, 1)
            z_way(p, u, 1, -1)

        def mid_way(p, u, sgn):
            (a_way if u == 0 else b_way)(p, u, 2 if sgn > 0 else 3, sgn)

        def last_way(p, u, sgn):
            (b_way if u == 0 else a_way)(p, u, 4 if sgn > 0 else 5, sgn)

        def mid_both(p, u):
            mid_way(p, u, 1)
            mid_way(p, u, -1)

        def last_both(p, u):
            last_way(p, u, 1)
            last_way(p, u, -1)

        def role(u):
            return (a, NA, b, NB) if u == 0 else (b, NB, a, NA)

        def at_role(u, mid, last, zz):
            return pos(core, mid, last, zz) if u == 0 else pos(core, last, mid, zz)

        def arrive(p, u):
            if start:
                copy(p, u, 6, device_of_twin).wait_recv()

        if U > 1:
            mid_both(own, 1)
        z_both(own, 0)
        last_both(own, 0)
        mid_both(own, 0)
        if U > 1:
            z_both(own, 1)
            last_both(own, 1)
        if start:
            send_targets()
        for u in range(U):
            twin(own, u)

        def across_mid(zz, u, extra):
            here, size, last, _ = role(u)
            for step in range(1, size):
                for sgn in (1, -1):
                    at = here + sgn * step

                    @pl.when((at >= 0) & (at < size))
                    def _():
                        p = at_role(u, at, last, zz)
                        arrive(p, u)
                        mid_way(p, u, -sgn)
                        if extra:
                            z_both(p, u)
                        last_both(p, u)
                        twin(p, u)

        def sides(s, fn):
            @pl.loop(0, 2)
            def _(side):
                zz = z + (1 - 2 * side) * s

                @pl.when((zz >= 0) & (zz < Z) & ((s > 0) | (side == 0)))
                def _():
                    fn(zz, side)

        if U > 1:
            across_mid(z, 1, True)

        def from_z(p, u, side):
            arrive(p, u)
            put(p, u, 1 - side, z + 2 * side - 1, Z, lambda w: device(core, a, b, w))

        def z_first(zz, side):
            p = pos(core, a, b, zz)
            from_z(p, 0, side)
            mid_both(p, 0)
            last_both(p, 0)
            twin(p, 0)

        def z_second(zz, side, k, u):
            here, size, last, _ = role(u)
            q = at_role(u, (here + k) % size, last, zz)
            from_z(q, u, side)
            last_both(q, u)
            twin(q, u)

        def late(zz, side):
            across_mid(zz, 0, False)

        def b_arrivals(zz, side):
            for u in range(U):
                here, size, last, length = role(u)

                @pl.loop(0, size)
                def _(k):
                    for step in range(1, length):
                        for sgn in (1, -1):
                            at = last + sgn * step

                            @pl.when((at >= 0) & (at < length))
                            def _():
                                p = at_role(u, (here + k) % size, at, zz)
                                arrive(p, u)
                                last_way(p, u, -sgn)
                                twin(p, u)

        @pl.loop(1, Z + 2)
        def _(s):
            @pl.when(s < Z)
            def _():
                sides(s, z_first)
                for u in range(1, U):
                    @pl.loop(0, role(u)[1])
                    def _(k):
                        sides(s, lambda zz, side: z_second(zz, side, k, u))

            @pl.when(s <= Z)
            def _():
                sides(s - 1, late)

            @pl.when(s >= 2)
            def _():
                sides(s - 2, b_arrivals)
                if start:
                    @pl.when(s == 2)
                    def _():
                        load_emb.wait()
                        few = tgs.at[pl.ds(0, N - 1)]
                        pltpu.make_async_remote_copy(
                            few, few, small_send.at[0], small_recv.at[0], device_id=device_of_twin, device_id_type=MESH
                        ).wait()

                    sides(s - 2, batch)

    device_of_twin = ((g // CORES) * CORES + 1 - core, v)

    blocks = NA * NB
    first_id = (v * lax.axis_size("grp") + g) * shard

    def batch(zz, side):
        @pl.loop(0, CORES)
        def _(k):
            c = (core + k) % CORES
            base = pos(c, 0, 0, zz)

            @pl.when(k == 1)
            def _():
                @pl.loop(0, blocks * U)
                def _(i):
                    copy(base + i // U, i % U, 6, device_of_twin).wait_recv()

            where_to = [natural(c, i % NA, i // NA, zz) for i in range(blocks)]
            wanted = jnp.concatenate([tgs[w] for w in where_to], axis=1)
            tokens = blocks * rows

            def step(i, carry):
                start = pl.multiple_of(i * chunk, chunk)
                logits = lax.dot_general(
                    emb[pl.ds(start, chunk), :],
                    buf[pl.ds(base, blocks)].reshape(tokens, depth),
                    (((1,), (1,)), ((), ())),
                    preferred_element_type=jnp.float32,
                )
                capped = soft_cap * jnp.tanh(logits * (1.0 / soft_cap))
                ids = lax.broadcasted_iota(jnp.int32, (chunk, tokens), 0)
                hit = ids == (wanted - (first_id + start))
                return (
                    carry[0] + jnp.sum(jnp.exp(capped - soft_cap), axis=0, keepdims=True),
                    carry[1] + jnp.sum(jnp.where(hit, capped, 0.0), axis=0, keepdims=True),
                )

            zero = jnp.zeros((1, tokens), jnp.float32)
            total, picked = lax.fori_loop(0, shard // chunk, step, (zero, zero))
            for i, w in enumerate(where_to):
                sums[w, 0:1, :] = total[:, i * rows : (i + 1) * rows]
                sums[w, 1:2, :] = picked[:, i * rows : (i + 1) * rows]
            for w in where_to:
                @pl.when(w != me)
                def _():
                    pltpu.make_async_remote_copy(
                        sums.at[w], parts.at[me], small_send.at[1], small_recv.at[1],
                        device_id=(w // V, w % V), device_id_type=MESH,
                    ).start()

    traverse(True)

    def exchange(source_of, dest, which):
        @pl.loop(1, N)
        def _(k):
            dev, t = other(k)
            pltpu.make_async_remote_copy(
                source_of(t), dest.at[me], small_send.at[which], small_recv.at[which], device_id=dev, device_id_type=MESH
            ).start()

    def settle(dest, which):
        few = dest.at[pl.ds(0, N - 1)]
        pltpu.make_async_remote_copy(
            few, few, small_send.at[which], small_recv.at[which], device_id=device_of_twin, device_id_type=MESH
        ).wait()

    parts[me] = sums[me]
    settle(parts, 1)

    both = jnp.sum(parts[...], axis=0)
    lse = soft_cap + jnp.log(both[0:1, :])
    zterm = zloss_coef * lse * lse
    loss_ref[...] = lse - both[1:2, :] + zterm
    width = docs.shape[2]
    of_doc = lax.broadcasted_iota(jnp.int32, (n_docs, rows), 0) == seg_ref[...]
    column = jnp.sum(jnp.where(of_doc, zterm, 0.0), axis=1, keepdims=True)
    diagonal = lax.broadcasted_iota(jnp.int32, (n_docs, width), 0) == lax.broadcasted_iota(
        jnp.int32, (n_docs, width), 1
    )
    docs[me] = jnp.sum(jnp.where(diagonal, column, 0.0), axis=0, keepdims=True)
    exchange(lambda t: docs.at[me], docs, 2)
    traverse(False)
    settle(docs, 2)
    doc_ref[...] = jnp.sum(docs[...], axis=0)[:, :n_docs]


def solution(mesh):
    G, V = mesh.shape["grp"], mesh.shape["vocab"]
    N = G * V
    Y = G // CORES
    X = Y if V % Y == 0 else 1
    Z = V // X
    n_docs = DOC_GRP * G

    def body(hidden, embedding, targets, segments):
        rows, depth = hidden.shape
        shard = embedding.shape[0]
        U = 2 if rows % 32 == 0 else 1
        chunk = min(1024, shard)
        dims = (X, Y, Z, X, V, N, U, chunk)
        width = -(-n_docs // LANES) * LANES
        any_spec = pl.BlockSpec(memory_space=pl.ANY)
        vmem = pl.BlockSpec(memory_space=pltpu.VMEM)
        loss, doc = pl.pallas_call(
            functools.partial(kernel, dims),
            out_shape=(
                jax.ShapeDtypeStruct((1, rows), jnp.float32),
                jax.ShapeDtypeStruct((1, n_docs), jnp.float32),
            ),
            in_specs=[any_spec, any_spec, vmem, vmem],
            out_specs=(vmem, vmem),
            scratch_shapes=[
                pltpu.VMEM((N, rows, depth), jnp.bfloat16),
                pltpu.VMEM((shard, depth), jnp.bfloat16),
                pltpu.VMEM((N, 1, rows), jnp.int32),
                pltpu.VMEM((N, 2, rows), jnp.float32),
                pltpu.VMEM((N, 2, rows), jnp.float32),
                pltpu.VMEM((N, 1, width), jnp.float32),
                pltpu.SemaphoreType.DMA((3,)),
                pltpu.SemaphoreType.DMA((N * U, 7)),
                pltpu.SemaphoreType.DMA((N * U,)),
                pltpu.SemaphoreType.DMA((3,)),
                pltpu.SemaphoreType.DMA((3,)),
            ],
            compiler_params=pltpu.CompilerParams(
                collective_id=0, has_side_effects=True, vmem_limit_bytes=60 * 1024 * 1024
            ),
        )(hidden, embedding, targets.reshape(1, rows), segments.reshape(1, rows))
        return (loss.reshape(rows), doc.reshape(n_docs))

    return jax.shard_map(
        body,
        mesh=mesh,
        in_specs=(
            P(("grp", "vocab"), None),
            P(("vocab", "grp"), None),
            P(("grp", "vocab")),
            P(("grp", "vocab")),
        ),
        out_specs=(P(("grp", "vocab")), P()),
        check_vma=False,
    )
```
